32 devices in a mesh: rep: 2 (over z, core), dp: 16 (over x, y).
Axes of the slice: x: 4, y: 4, z: 1, core: 2. Of those that a mesh axis runs over, the one named last changes fastest.
The devices are a block of a 4x4x8 slice.
Arguments:
- x: bfloat16 [32, 4096, 512], P(('rep', 'dp')), parts along dimension 0
- dy: bfloat16 [32, 4096, 512], P(('rep', 'dp')), parts along dimension 0
- w_gate: bfloat16 [2, 512, 2048], P(None, 'dp')
- w_up: bfloat16 [2, 512, 2048], P(None, 'dp')
- w_down: bfloat16 [2, 2048, 512], P(None, 'dp')
- m_w_gate: float32 [2, 512, 2048], P(None, 'dp')
- m_w_up: float32 [2, 512, 2048], P(None, 'dp')
- m_w_down: float32 [2, 2048, 512], P(None, 'dp')
- v_w_gate: float32 [2, 512, 2048], P(None, 'dp')
- v_w_up: float32 [2, 512, 2048], P(None, 'dp')
- v_w_down: float32 [2, 2048, 512], P(None, 'dp')
Outputs:
- output 1: bfloat16 [4, 512, 2048], P('rep', 'dp'), parts along dimension 0
- output 2: bfloat16 [4, 512, 2048], P('rep', 'dp'), parts along dimension 0
- output 3: bfloat16 [4, 2048, 512], P('rep', 'dp'), parts along dimension 0
- output 4: float32 [4, 512, 2048], P('rep', 'dp'), parts along dimension 0
- output 5: float32 [4, 512, 2048], P('rep', 'dp'), parts along dimension 0
- output 6: float32 [4, 2048, 512], P('rep', 'dp'), parts along dimension 0
- output 7: float32 [4, 512, 2048], P('rep', 'dp'), parts along dimension 0
- output 8: float32 [4, 512, 2048], P('rep', 'dp'), parts along dimension 0
- output 9: float32 [4, 2048, 512], P('rep', 'dp'), parts along dimension 0
There are 2 independent parts. The reference program is written for one: setup_inputs(seed, part) draws one part's arguments, and reference() takes and returns one part's arrays. A program takes and returns all parts, laid end to end along the dimension named above; an argument that names none is the same for every part.
All inputs are finite; a program needn't handle non-finite values.
Results may differ from the reference program's by a relative error of at most 0.02.
Values are sent between devices in bfloat16 or wider.
A program may use at most 768 MiB of HBM per device.

```python
import jax
import jax.numpy as jnp
from jax import lax

SEQUENCES = 16
TOKENS = 4096
D = 512
FF = 2048
LAYERS = 2
NAMES = ("w_gate", "w_up", "w_down")
SHAPES = {"w_gate": (LAYERS, D, FF), "w_up": (LAYERS, D, FF), "w_down": (LAYERS, FF, D)}


def bump(key, n, height):
    away = (jnp.arange(n, dtype=jnp.int32) - jax.random.randint(key, (), 0, n, jnp.int32)) % n
    return jnp.where(away < n // 8, height, 1.0)


def together(key, own, strength):
    shared = jax.random.normal(key, own.shape[1:], jnp.float32)
    return (own + strength * shared) * lax.rsqrt(1 + strength * strength)


def setup_inputs(seed: int = 0, part: int = 0) -> dict:
    kx, kdy, ka, kb, kz, kf, kh, kl, *keys = jax.random.split(jax.random.key(seed), 8 + 3 * len(NAMES))
    kx, kdy, ka, kb = (jax.random.fold_in(k, part) for k in (kx, kdy, ka, kb))
    kw, km, kv = (keys[i::3] for i in range(3))
    shape = (SEQUENCES, TOKENS, D)
    much_x, much_dy = jax.random.uniform(kz, (2,), jnp.float32, 0.0, 1.0)
    loud = 2.0 ** jax.random.uniform(jax.random.fold_in(kz, 1), (), jnp.float32, -1.0, 2.0)
    layers = 2.0 ** jax.random.uniform(kl, (LAYERS, 1, 1), jnp.float32, -1.0, 1.0)
    x = together(ka, jax.random.normal(kx, shape, jnp.float32), much_x) * bump(kf, D, 4.0)
    dy = together(kb, jax.random.normal(kdy, shape, jnp.float32), much_dy)
    drawn = {"x": x.astype(jnp.bfloat16), "dy": (loud * dy * (SEQUENCES * TOKENS) ** -0.5).astype(jnp.bfloat16)}
    for key, name in zip(kw, NAMES, strict=True):
        w = jax.random.normal(key, SHAPES[name], jnp.float32) * SHAPES[name][1] ** -0.5
        drawn[name] = (w * {"w_gate": 1.0, "w_up": bump(kh, FF, 4.0), "w_down": layers}[name]).astype(jnp.bfloat16)
    for key, name in zip(km, NAMES, strict=True):
        drawn[f"m_{name}"] = 0.1 * jax.random.normal(key, SHAPES[name], jnp.float32)
    for key, name in zip(kv, NAMES, strict=True):
        drawn[f"v_{name}"] = jax.random.uniform(key, SHAPES[name], jnp.float32, 0.005, 0.015)
    return drawn


def matmul(a, w):
    return jnp.dot(a, w, preferred_element_type=jnp.float32).astype(jnp.bfloat16)


def normed(h):
    wide = h.astype(jnp.float32)
    scale = lax.rsqrt(jnp.mean(wide**2, -1, keepdims=True) + 1e-6)
    return (wide * scale).astype(jnp.bfloat16)


def layer(h, w):
    a = normed(h)
    gate = jnp.dot(a, w["w_gate"], preferred_element_type=jnp.float32)
    up = jnp.dot(a, w["w_up"], preferred_element_type=jnp.float32)
    return h + matmul((jax.nn.silu(gate) * up).astype(jnp.bfloat16), w["w_down"])


def adamw(w, m, v, g):
    m = 0.9 * m + 0.1 * g
    v = 0.95 * v + 0.05 * g * g
    step = m * lax.rsqrt(v + 1e-8) + 0.1 * w
    return (w - 0.02 * step).astype(jnp.bfloat16), m, v


def stack(weights, h):
    return lax.scan(lambda h, w: (layer(h, w), None), h, weights)[0]


def reference(x, dy, w_gate, w_up, w_down, m_w_gate, m_w_up, m_w_down, v_w_gate, v_w_up, v_w_down):
    weights = dict(zip(NAMES, (w_gate, w_up, w_down), strict=True))

    def take(so_far, sequence):
        h, by_y = sequence
        _, back = jax.vjp(lambda w: stack(w, h), weights)
        return jax.tree.map(lambda total, term: total + term.astype(jnp.float32), so_far, back(by_y)[0]), None

    none_yet = {name: jnp.zeros(w.shape, jnp.float32) for name, w in weights.items()}
    by_weights, _ = lax.scan(take, none_yet, (x, dy))
    gradients = [by_weights[name].astype(jnp.bfloat16).astype(jnp.float32) for name in NAMES]
    new = [
        adamw(w.astype(jnp.float32), m, v, g)
        for w, m, v, g in zip((w_gate, w_up, w_down), (m_w_gate, m_w_up, m_w_down), (v_w_gate, v_w_up, v_w_down), gradients, strict=True)
    ]
    return tuple(one[which] for which in range(3) for one in new)
```

```python
import functools
import math

import jax, jax.numpy as jnp
from jax import lax
from jax.experimental import pallas as pl
from jax.experimental.pallas import tpu as pltpu
from jax.sharding import PartitionSpec as P

BF, F32 = jnp.bfloat16, jnp.float32
VM = 63 * 2**20

def dot(a, b, ca=1, cb=0):
    return lax.dot_general(a, b, (((ca,), (cb,)), ((), ())), preferred_element_type=F32)

def scale_of(wide):
    return lax.rsqrt(jnp.mean(wide * wide, -1, keepdims=True) + 1e-6)

def over(tokens, tile, unroll, body):
    def step(t, _):
        body(pl.ds(pl.multiple_of(t * tile, tile), tile))
        return 0
    lax.fori_loop(0, tokens // tile, step, 0, unroll=unroll)

def prepare(h_ref, a_ref, total):
    def first(rows):
        wide = h_ref[rows, :].astype(F32)
        a_ref[rows, :] = (wide * scale_of(wide)).astype(BF)
        if total is not None:
            total[rows, :] = jnp.zeros((rows.size, total.shape[1]), F32)
    over(h_ref.shape[0], 256, 1, first)

def forward_kernel(h_ref, wg_ref, wu_ref, wd_ref, out_ref, a_ref, total, *, chunks, tile, unroll):
    c = pl.program_id(0)
    pl.when(c == 0)(lambda: prepare(h_ref, a_ref, total))
    def main(rows):
        a = a_ref[rows, :]
        gate = dot(a, wg_ref[...])
        up = dot(a, wu_ref[...])
        act = (gate * jax.nn.sigmoid(gate) * up).astype(BF)
        total[rows, :] += dot(act, wd_ref[...])
    over(h_ref.shape[0], tile, unroll, main)
    @pl.when(c == chunks - 1)
    def _():
        def last(rows):
            out_ref[rows, :] = h_ref[rows, :] + total[rows, :].astype(BF)
        over(h_ref.shape[0], 256, 1, last)

def forward(h, wg, wu, wd, tile=512, chunk=512, unroll=1):
    tokens, d = h.shape; ff = wg.shape[1]
    chunks = ff // chunk
    tok = pl.BlockSpec((tokens, d), lambda c: (0, 0), pipeline_mode=pl.Buffered(1))
    col = pl.BlockSpec((d, chunk), lambda c: (0, c))
    return pl.pallas_call(
        functools.partial(forward_kernel, chunks=chunks, tile=tile, unroll=unroll),
        grid=(chunks,),
        in_specs=[tok, col, col, pl.BlockSpec((chunk, d), lambda c: (c, 0))],
        out_specs=tok,
        out_shape=jax.ShapeDtypeStruct(h.shape, BF),
        scratch_shapes=[pltpu.VMEM((tokens, d), BF), pltpu.VMEM((tokens, d), F32)],
        compiler_params=pltpu.CompilerParams(dimension_semantics=("arbitrary",), vmem_limit_bytes=VM),
        cost_estimate=pl.CostEstimate(flops=6 * tokens * d * ff, bytes_accessed=4 * tokens * d * chunks, transcendentals=tokens * ff),
        name="forward",
    )(h, wg, wu, wd)

def backward_kernel(h_ref, dy_ref, wg_ref, wu_ref, wd_ref, *rest, chunks, tile, unroll, carry):
    if carry:
        dh_ref, gg_ref, gu_ref, gd_ref, a_ref, sg, su, sd, total = rest
    else:
        gg_ref, gu_ref, gd_ref, a_ref, sg, su, sd = rest
        total = None
    c = pl.program_id(0)
    pl.when(c == 0)(lambda: prepare(h_ref, a_ref, total))
    sg[...] = jnp.zeros_like(sg); su[...] = jnp.zeros_like(su); sd[...] = jnp.zeros_like(sd)
    def main(rows):
        a, dy = a_ref[rows, :], dy_ref[rows, :]
        gate = dot(a, wg_ref[...])
        up = dot(a, wu_ref[...])
        dact = dot(dy, wd_ref[...], 1, 1).astype(BF).astype(F32)
        sig = jax.nn.sigmoid(gate)
        silu = gate * sig
        act = (silu * up).astype(BF)
        dup = (dact * silu).astype(BF)
        dgate = (dact * up * (sig + silu * (1 - sig))).astype(BF)
        sd[...] += dot(act, dy, 0, 0)
        sg[...] += dot(a, dgate, 0, 0)
        su[...] += dot(a, dup, 0, 0)
        if carry:
            total[rows, :] += dot(dgate, wg_ref[...], 1, 1) + dot(dup, wu_ref[...], 1, 1)
    over(h_ref.shape[0], tile, unroll, main)
    gd_ref[...] = sd[...].astype(BF); gg_ref[...] = sg[...].astype(BF); gu_ref[...] = su[...].astype(BF)
    if carry:
        @pl.when(c == chunks - 1)
        def _():
            def last(rows):
                wide = h_ref[rows, :].astype(F32)
                scale = scale_of(wide)
                da = total[rows, :].astype(BF).astype(F32)
                dwide = scale * (da - wide * (scale * scale * jnp.mean(da * wide, -1, keepdims=True)))
                dh_ref[rows, :] = dy_ref[rows, :] + dwide.astype(BF)
            over(h_ref.shape[0], 256, 1, last)

def backward(h, dy, wg, wu, wd, carry, tile=256, chunk=512, unroll=2):
    tokens, d = h.shape; ff = wg.shape[1]
    chunks = ff // chunk
    tok = pl.BlockSpec((tokens, d), lambda c: (0, 0), pipeline_mode=pl.Buffered(1))
    col = pl.BlockSpec((d, chunk), lambda c: (0, c))
    row = pl.BlockSpec((chunk, d), lambda c: (c, 0))
    outs = [jax.ShapeDtypeStruct(wg.shape, BF), jax.ShapeDtypeStruct(wu.shape, BF), jax.ShapeDtypeStruct(wd.shape, BF)]
    ospecs = [col, col, row]
    scratch = [pltpu.VMEM((tokens, d), BF), pltpu.VMEM((d, chunk), F32), pltpu.VMEM((d, chunk), F32), pltpu.VMEM((chunk, d), F32)]
    if carry:
        outs, ospecs = [jax.ShapeDtypeStruct(h.shape, BF)] + outs, [tok] + ospecs
        scratch += [pltpu.VMEM((tokens, d), F32)]
    return pl.pallas_call(
        functools.partial(backward_kernel, chunks=chunks, tile=tile, unroll=unroll, carry=carry),
        grid=(chunks,), in_specs=[tok, tok, col, col, row], out_specs=ospecs, out_shape=outs, scratch_shapes=scratch,
        compiler_params=pltpu.CompilerParams(dimension_semantics=("arbitrary",), vmem_limit_bytes=VM),
        cost_estimate=pl.CostEstimate(flops=(16 if carry else 12) * tokens * d * ff, bytes_accessed=4 * tokens * d * chunks, transcendentals=tokens * ff),
        name="backward_carry" if carry else "backward",
    )(h, dy, wg, wu, wd)


MESH = pl.DeviceIdType.MESH


class Place:
    def __init__(self, side, send_sems, recv_sems):
        self.side, self.send_sems, self.recv_sems, self.used = side, send_sems, recv_sems, 0
        me, rep = lax.axis_index("dp"), lax.axis_index("rep")
        self.at = (lax.div(me, side), lax.rem(me, side))
        self.parity = lax.rem(rep, 2)
        self.partner = rep + 1 - 2 * self.parity

    def along(self, axis, step):
        return lax.rem(self.at[axis] + step + self.side, self.side)

    def peer(self, axis, step):
        there = self.along(axis, step)
        return {"dp": there * self.side + self.at[1] if axis == 0 else self.at[0] * self.side + there}

    def greet(self, partner):
        barrier = pltpu.get_barrier_semaphore()
        peers = [self.peer(axis, step) for axis in (0, 1) for step in range(1, self.side)]
        peers += [{"rep": self.partner}] if partner else []
        for peer in peers:
            pl.semaphore_signal(barrier, inc=1, device_id=peer, device_id_type=MESH)
        pl.semaphore_wait(barrier, len(peers))

    def copy(self, src, dst, device):
        number, self.used = self.used, self.used + 1
        return pltpu.make_async_remote_copy(
            src_ref=src, dst_ref=dst, send_sem=self.send_sems.at[number], recv_sem=self.recv_sems.at[number], device_id=device, device_id_type=MESH
        )


def halves(parity, rows):
    return pl.ds(pl.multiple_of(parity * rows, rows), rows)


def gathering(place, blocks, wholes, local_sems):
    side, parity = place.side, place.parity
    parts = []
    for n, (block, whole) in enumerate(zip(blocks, wholes, strict=True)):
        half = block.shape[0] // 2
        if n < 2:
            parts.append((n, block, whole, halves(parity, half)))
        else:
            for axis in (0, 1):
                parts.append((axis, block, whole, pl.ds(pl.multiple_of(parity * half + axis * (half // 2), half // 2), half // 2)))

    def spot(whole, axis, i, j, rows):
        a, b = place.along(axis, -i), place.along(1 - axis, -j)
        return whole.at[a, b, rows] if axis == 0 else whole.at[b, a, rows]

    kept = []
    for n, (axis, block, whole, rows) in enumerate(parts):
        kept.append(pltpu.make_async_copy(block.at[rows], spot(whole, axis, 0, 0, rows), local_sems.at[n]))
        kept[-1].start()
    direct = [{} for _ in parts]
    for step in range(1, side):
        for n, (axis, block, whole, rows) in enumerate(parts):
            for way, which in ((axis, "near"), (1 - axis, "far")):
                copy = place.copy(block.at[rows], spot(whole, axis, 0, 0, rows), place.peer(way, step))
                copy.start()
                direct[n][which, step] = copy
    yield
    handed = [[] for _ in parts]
    for step in range(1, side):
        for n, (axis, block, whole, rows) in enumerate(parts):
            direct[n]["near", step].wait_recv()
            for other in range(1, side):
                here = spot(whole, axis, step, 0, rows)
                copy = place.copy(here, here, place.peer(1 - axis, other))
                copy.start()
                handed[n].append(copy)
    yield
    for n in range(len(parts)):
        kept[n].wait()
        for step in range(1, side):
            direct[n]["far", step].wait_recv()
        for copy in handed[n]:
            copy.wait_recv()
        if n == 2:
            continue
        block, whole = parts[n][1:3]
        mine = whole.at[:, :, halves(parity, block.shape[0] // 2)]
        across = place.copy(mine, mine, {"rep": place.partner})
        across.start()
        handed.append([across])
    yield
    for n in range(len(parts)):
        for copy in direct[n].values():
            copy.wait_send()
        for copy in handed[n]:
            copy.wait_send()
    for (across,) in handed[len(parts) :]:
        across.wait_send()
        across.wait_recv()


def gather_kernel(side, layers, *refs):
    blocks, wholes, (send_sems, recv_sems, local_sems) = refs[: 3 * layers], refs[3 * layers : 6 * layers], refs[6 * layers :]
    place = Place(side, send_sems, recv_sems)
    place.greet(True)
    runs = [gathering(place, blocks[3 * n : 3 * n + 3], wholes[3 * n : 3 * n + 3], local_sems.at[n]) for n in range(layers)]
    for _ in range(4):
        for run in runs:
            next(run, None)


def gather(side, blocks, number):
    layers = len(blocks) // 3
    copies = layers * (4 * (side * side - 1) + 3)
    return pl.pallas_call(
        functools.partial(gather_kernel, side, layers),
        in_specs=[pl.BlockSpec(memory_space=pltpu.VMEM)] * len(blocks),
        out_specs=[pl.BlockSpec(memory_space=pltpu.HBM)] * len(blocks),
        out_shape=[jax.ShapeDtypeStruct((side, side, *b.shape), b.dtype) for b in blocks],
        scratch_shapes=[pltpu.SemaphoreType.DMA((copies,)), pltpu.SemaphoreType.DMA((copies,)), pltpu.SemaphoreType.DMA((layers, 4))],
        compiler_params=pltpu.CompilerParams(collective_id=number, has_side_effects=True),
        name=f"gather_{number}",
    )(*blocks)


def scatter_parts(shapes):
    parts = []
    for n, (rows, columns) in enumerate(shapes):
        parts += [(n, n, 0, rows, columns)] if n < 2 else [(axis, n, axis * (rows // 2), rows // 2, columns) for axis in (0, 1)]
    return parts


def scatter_scratch(side, shapes):
    scratch = []
    for _, _, _, rows, columns in scatter_parts(shapes):
        scratch += [pltpu.VMEM((side, side, rows, columns), BF), pltpu.VMEM((side, rows, columns), BF), pltpu.VMEM((side - 1, rows, columns), BF)]
    return scratch + [pltpu.SemaphoreType.DMA((len(scratch) // 3,))]


def scattering(place, terms, outs, scratch):
    side = place.side
    local_sems = scratch[-1]
    parts = scatter_parts([out.shape for out in outs])

    def wide(ref, *index):
        return ref[index].astype(F32)

    work = []
    for n, (axis, matrix, start, rows, columns) in enumerate(parts):
        within = pl.ds(start, rows)
        first, partial, second = scratch[3 * n : 3 * n + 3]

        def line(step, axis=axis, term=terms[matrix], within=within):
            there = place.along(axis, step)
            return term.at[there, :, within] if axis == 0 else term.at[:, there, within]

        own = pltpu.make_async_copy(line(0), first.at[0], local_sems.at[n])
        own.start()
        copies = []
        for step in range(1, side):
            copies.append(place.copy(line(step), first.at[step], place.peer(axis, step)))
            copies[-1].start()
        work.append((axis, outs[matrix], within, first, partial, second, own, copies))
    yield
    later = []
    for axis, out, within, first, partial, second, own, copies in work:
        own.wait()
        for copy in copies:
            copy.wait_recv()

        def add(k, _, first=first, partial=partial):
            partial[k] = sum(wide(first, step, k) for step in range(side)).astype(BF)
            return 0

        lax.fori_loop(0, side, add, 0)
        later.append([])
        for step in range(1, side):
            copy = place.copy(partial.at[place.along(1 - axis, step)], second.at[step - 1], place.peer(1 - axis, step))
            copy.start()
            later[-1].append(copy)
    yield
    for (axis, out, within, first, partial, second, own, copies), more in zip(work, later, strict=True):
        for copy in more:
            copy.wait_recv()
        total = wide(partial, place.at[1 - axis])
        for step in range(side - 1):
            total += wide(second, step)
        out[within, :] = total.astype(BF)
        for copy in copies + more:
            copy.wait_send()


def scatter_kernel(side, layers, *refs):
    terms, outs, scratch = refs[: 3 * layers], refs[3 * layers : 6 * layers], refs[6 * layers :]
    place = Place(side, *scratch[:2])
    place.greet(False)
    each = (len(scratch) - 2) // layers
    runs = [scattering(place, terms[3 * n : 3 * n + 3], outs[3 * n : 3 * n + 3], scratch[2 + each * n : 2 + each * (n + 1)]) for n in range(layers)]
    for _ in range(3):
        for run in runs:
            next(run, None)


def scatter(side, terms, number):
    layers = len(terms) // 3
    shapes = [(t.shape[0] // side**2, t.shape[1]) for t in terms]
    copies = layers * 4 * 2 * (side - 1)
    scratch = [pltpu.SemaphoreType.DMA((copies,)), pltpu.SemaphoreType.DMA((copies,))]
    for n in range(layers):
        scratch += scatter_scratch(side, shapes[3 * n : 3 * n + 3])
    return pl.pallas_call(
        functools.partial(scatter_kernel, side, layers),
        in_specs=[pl.BlockSpec(memory_space=pltpu.HBM)] * len(terms),
        out_specs=[pl.BlockSpec(memory_space=pltpu.VMEM)] * len(terms),
        out_shape=[jax.ShapeDtypeStruct(s, BF) for s in shapes],
        scratch_shapes=scratch,
        compiler_params=pltpu.CompilerParams(collective_id=number, has_side_effects=True, vmem_limit_bytes=48 * 2**20),
        name=f"scatter_{number}",
    )(*(t.reshape(side, side, *s) for t, s in zip(terms, shapes, strict=True)))


NAMES = ("w_gate", "w_up", "w_down")


def adamw(w, m, v, g):
    m = 0.9 * m + 0.1 * g
    v = 0.95 * v + 0.05 * g * g
    step = m * lax.rsqrt(v + 1e-8) + 0.1 * w
    return (w - 0.02 * step).astype(BF), m, v


def solution(mesh):
    side = math.isqrt(mesh.shape["dp"])

    def step(x, dy, *arrays):
        weights, m, v = (arrays[i : i + 3] for i in (0, 3, 6))
        layers = weights[0].shape[0]
        h, dh = x[0], dy[0]
        wholes = gather(side, [w[number] for number in range(layers) for w in weights], 1)
        wholes = [w.reshape(-1, w.shape[-1]) for w in wholes]
        wholes = [wholes[3 * number : 3 * number + 3] for number in range(layers)]
        kept = [h]
        for number in range(layers - 1):
            kept.append(forward(kept[-1], *wholes[number]))
        terms = [None] * layers
        for number in reversed(range(layers)):
            if number:
                dh, *terms[number] = backward(kept[number], dh, *wholes[number], True)
            else:
                terms[number] = backward(kept[number], dh, *wholes[number], False)
        mine = scatter(side, sum((list(t) for t in terms), []), 2)
        gradients = [jnp.stack(mine[i::3]).astype(F32) for i in range(3)]
        new = [adamw(w.astype(F32), m, v, g) for w, m, v, g in zip(weights, m, v, gradients, strict=True)]
        return tuple(one[which] for which in range(3) for one in new)

    states, cut = P(("rep", "dp"), None, None), P(None, "dp", None)
    return jax.shard_map(
        step,
        mesh=mesh,
        in_specs=(states, states) + (cut,) * 9,
        out_specs=(P("rep", "dp", None),) * 9,
        check_vma=False,
    )
```

```python
import functools
import math

import jax
import jax.numpy as jnp
from jax import lax
from jax.experimental import pallas as pl
from jax.experimental.pallas import tpu as pltpu
from jax.sharding import PartitionSpec as P

BF, F32 = jnp.bfloat16, jnp.float32
VMEM_LIMIT = 63 * 2**20
MESH = pl.DeviceIdType.MESH
HBM = pl.BlockSpec(memory_space=pltpu.HBM)
VMEM = pl.BlockSpec(memory_space=pltpu.VMEM)
DMA = pltpu.SemaphoreType.DMA


class Place:
    def __init__(self, side, send_sems, recv_sems):
        self.side, self.send_sems, self.recv_sems = side, send_sems, recv_sems
        me, rep = lax.axis_index("dp"), lax.axis_index("rep")
        self.at = (lax.div(me, side), lax.rem(me, side))
        self.parity = lax.rem(rep, 2)
        self.partner = {"rep": rep + 1 - 2 * self.parity}

    def along(self, axis, step):
        return lax.rem(self.at[axis] + step + self.side, self.side)

    def peer(self, axis, step):
        there = self.along(axis, step)
        return {"dp": there * self.side + self.at[1] if axis == 0 else self.at[0] * self.side + there}

    def greet(self, partner):
        barrier = pltpu.get_barrier_semaphore()
        peers = [self.peer(axis, step) for axis in (0, 1) for step in range(1, self.side)]
        peers += [self.partner] if partner else []
        for peer in peers:
            pl.semaphore_signal(barrier, inc=1, device_id=peer, device_id_type=MESH)
        pl.semaphore_wait(barrier, len(peers))

    def copy(self, number, src, dst, device):
        return pltpu.make_async_remote_copy(
            src_ref=src, dst_ref=dst, send_sem=self.send_sems.at[number], recv_sem=self.recv_sems.at[number], device_id=device, device_id_type=MESH
        )


def span(start, size):
    return pl.ds(pl.multiple_of(start * size, size), size)


class Gathering:
    @staticmethod
    def copies(side):
        return 4 * (side * side - 1) + 3

    def __init__(self, place, blocks, wholes, local_sems):
        self.place, self.blocks, self.wholes, self.local_sems = place, blocks, wholes, local_sems

    def made(self):
        place, side, parity = self.place, self.place.side, self.place.parity
        parts = []
        for n, block in enumerate(self.blocks):
            half = block.shape[0] // 2
            if n < 2:
                parts.append((n, n, span(parity, half)))
            else:
                parts += [(axis, n, span(2 * parity + axis, half // 2)) for axis in (0, 1)]

        def spot(matrix, axis, behind, rows):
            a, b = place.along(axis, -behind), place.at[1 - axis]
            return self.wholes[matrix].at[a, b, rows] if axis == 0 else self.wholes[matrix].at[b, a, rows]

        kept, near, far, handed, number = [], {}, {}, {}, 0
        for n, (axis, matrix, rows) in enumerate(parts):
            src, own = self.blocks[matrix].at[rows], spot(matrix, axis, 0, rows)
            kept.append(pltpu.make_async_copy(src, own, self.local_sems.at[n]))
            for step in range(1, side):
                near[n, step] = place.copy(number, src, own, place.peer(axis, step))
                far[n, step] = place.copy(number + 1, src, own, place.peer(1 - axis, step))
                number += 2
                here = spot(matrix, axis, step, rows)
                for other in range(1, side):
                    handed[n, step, other] = place.copy(number, here, here, place.peer(1 - axis, other))
                    number += 1
        across = []
        for block, whole in zip(self.blocks, self.wholes, strict=True):
            mine = whole.at[:, :, span(parity, block.shape[0] // 2)]
            across.append(place.copy(number, mine, mine, place.partner))
            number += 1
        return kept, near, far, handed, across

    def send(self):
        kept, near, far, _, _ = self.made()
        for copy in kept:
            copy.start()
        for step in range(1, self.place.side):
            for n in range(len(kept)):
                near[n, step].start()
                far[n, step].start()

    def hand_on(self):
        kept, near, _, handed, _ = self.made()
        for step in range(1, self.place.side):
            for n in range(len(kept)):
                near[n, step].wait_recv()
                for other in range(1, self.place.side):
                    handed[n, step, other].start()

    def swap(self):
        kept, _, far, handed, across = self.made()
        for n, copy in enumerate(kept):
            copy.wait()
            for (part, *_), other in [*far.items(), *handed.items()]:
                if part == n:
                    other.wait_recv()
            if n != 2:
                across[min(n, 2)].start()

    def finish(self):
        _, near, far, handed, across = self.made()
        for copy in [*near.values(), *far.values(), *handed.values()]:
            copy.wait_send()
        for copy in across:
            copy.wait_send()
            copy.wait_recv()


def gather_kernel(side, layer, g, u, d, g_whole, u_whole, d_whole, send_sems, recv_sems, local_sems):
    place = Place(side, send_sems, recv_sems)
    run = Gathering(place, [block.at[layer] for block in (g, u, d)], (g_whole, u_whole, d_whole), local_sems)
    place.greet(True)
    run.send()
    run.hand_on()
    run.swap()
    run.finish()


def wholes_of(side, weights):
    return [jax.ShapeDtypeStruct((side, side, *w.shape[1:]), w.dtype) for w in weights]


def gather_sems(side):
    copies = Gathering.copies(side)
    return [DMA((copies,)), DMA((copies,)), DMA((4,))]


def gather(side, layer, weights, number):
    return pl.pallas_call(
        functools.partial(gather_kernel, side, layer),
        in_specs=[VMEM] * 3,
        out_specs=[HBM] * 3,
        out_shape=wholes_of(side, weights),
        scratch_shapes=gather_sems(side),
        compiler_params=pltpu.CompilerParams(collective_id=number, has_side_effects=True),
        name=f"gather_{number}",
    )(*weights)


class Scattering:
    @staticmethod
    def parts(shapes):
        parts = []
        for n, (rows, columns) in enumerate(shapes):
            parts += [(n, n, 0, rows, columns)] if n < 2 else [(axis, n, axis * (rows // 2), rows // 2, columns) for axis in (0, 1)]
        return parts

    @staticmethod
    def copies(side, pieces):
        return (side - 1) * (2 * pieces + 2 + 4)

    @classmethod
    def scratch(cls, side, shapes):
        scratch = []
        for _, _, _, rows, columns in cls.parts(shapes):
            scratch += [pltpu.VMEM((side, side, rows, columns), BF), pltpu.VMEM((side, rows, columns), BF), pltpu.VMEM((side - 1, rows, columns), BF)]
        return scratch + [DMA((4,))]

    def __init__(self, place, terms, outs, scratch, pieces, base, local):
        self.place, self.terms, self.outs, self.pieces, self.base, self.local = place, terms, outs, pieces, base, local
        self.split = self.parts([out.shape for out in outs])
        self.first, self.partial, self.second, self.local_sems = scratch[0:12:3], scratch[1:12:3], scratch[2:12:3], scratch[12]

    def line(self, part, step, columns):
        axis, matrix, start, rows, _ = self.split[part]
        there, within = self.place.along(axis, step), pl.ds(start, rows)
        return self.terms[matrix].at[there, :, within, columns] if axis == 0 else self.terms[matrix].at[:, there, within, columns]

    def near(self, part, piece=0):
        steps, width = self.place.side - 1, self.split[part][4]
        if part < 2:
            columns, number = span(piece, width // self.pieces), self.base + steps * (part * self.pieces + piece)
        else:
            columns, number = pl.ds(0, width), self.base + steps * (2 * self.pieces + part - 2)
        axis = self.split[part][0]
        return [
            self.place.copy(number + step - 1, self.line(part, step, columns), self.first[part].at[step, :, :, columns], self.place.peer(axis, step))
            for step in range(1, steps + 1)
        ]

    def own(self, part):
        return pltpu.make_async_copy(self.line(part, 0, pl.ds(0, self.split[part][4])), self.first[part].at[0], self.local_sems.at[part])

    def far(self, part):
        steps, axis = self.place.side - 1, self.split[part][0]
        number = self.base + steps * (2 * self.pieces + 2 + part)
        return [
            self.place.copy(
                number + step - 1, self.partial[part].at[self.place.along(1 - axis, step)], self.second[part].at[step - 1], self.place.peer(1 - axis, step)
            )
            for step in range(1, steps + 1)
        ]

    def pieces_of(self, part):
        return range(self.pieces if part < 2 else 1)

    def send(self, part, piece=0):
        if not self.local:
            self.own(part).start()
        for copy in self.near(part, piece):
            copy.start()

    def add(self, part):
        axis, matrix, start, rows, _ = self.split[part]
        first, partial, side = self.first[part], self.partial[part], self.place.side
        if not self.local:
            self.own(part).wait()
        for piece in self.pieces_of(part):
            for copy in self.near(part, piece):
                copy.wait_recv()
        here, within = self.place.at[axis], pl.ds(start, rows)

        def one(k, _):
            if not self.local:
                total = first[0, k].astype(F32)
            else:
                total = (self.terms[matrix][here, k, within] if axis == 0 else self.terms[matrix][k, here, within]).astype(F32)
            for step in range(1, side):
                total += first[step, k].astype(F32)
            partial[k] = total.astype(BF)
            return 0

        lax.fori_loop(0, side, one, 0)
        for copy in self.far(part):
            copy.start()

    def finish(self, part):
        axis, matrix, start, rows, _ = self.split[part]
        for copy in self.far(part):
            copy.wait_recv()
        total = self.partial[part][self.place.at[1 - axis]].astype(F32)
        for step in range(self.place.side - 1):
            total += self.second[part][step].astype(F32)
        self.outs[matrix][pl.ds(start, rows), :] = total.astype(BF)
        for piece in self.pieces_of(part):
            for copy in self.near(part, piece):
                copy.wait_send()
        for copy in self.far(part):
            copy.wait_send()


def dot(a, b, ca=1, cb=0):
    return lax.dot_general(a, b, (((ca,), (cb,)), ((), ())), preferred_element_type=F32)


def scale_of(wide):
    return lax.rsqrt(jnp.mean(wide * wide, -1, keepdims=True) + 1e-6)


def over(tokens, tile, unroll, body):
    def step(t, _):
        body(span(t, tile))
        return 0

    lax.fori_loop(0, tokens // tile, step, 0, unroll=unroll)


def prepare(h_ref, a_ref, total):
    def first(rows):
        wide = h_ref[rows, :].astype(F32)
        a_ref[rows, :] = (wide * scale_of(wide)).astype(BF)
        if total is not None:
            total[rows, :] = jnp.zeros((rows.size, total.shape[1]), F32)

    over(h_ref.shape[0], 256, 1, first)


def forward_kernel(
    side, chunks, layer, h_ref, wg_ref, wu_ref, wd_ref, g, u, d, out_ref, g_whole, u_whole, d_whole, a_ref, total, send_sems, recv_sems, local_sems
):
    c = pl.program_id(0)
    place = Place(side, send_sems, recv_sems)
    run = Gathering(place, [block.at[layer] for block in (g, u, d)], (g_whole, u_whole, d_whole), local_sems)

    @pl.when(c == 0)
    def _():
        place.greet(True)
        run.send()
        prepare(h_ref, a_ref, total)

    pl.when(c == 1)(run.hand_on)
    pl.when(c == chunks - 1)(run.swap)

    def main(rows):
        a = a_ref[rows, :]
        gate = dot(a, wg_ref[...])
        up = dot(a, wu_ref[...])
        act = (gate * jax.nn.sigmoid(gate) * up).astype(BF)
        total[rows, :] += dot(act, wd_ref[...])

    over(h_ref.shape[0], 512, 1, main)

    @pl.when(c == chunks - 1)
    def _():
        def last(rows):
            out_ref[rows, :] = h_ref[rows, :] + total[rows, :].astype(BF)

        over(h_ref.shape[0], 256, 1, last)
        run.finish()


def blocks_of(h, wg, chunks):
    tokens, width = h.shape
    chunk = wg.shape[1] // chunks
    tok = pl.BlockSpec((tokens, width), lambda c: (0, 0), pipeline_mode=pl.Buffered(1))
    return tok, pl.BlockSpec((width, chunk), lambda c: (0, c)), pl.BlockSpec((chunk, width), lambda c: (c, 0))


def forward(side, h, whole, weights, layer, number):
    (tokens, width), hidden, chunks = h.shape, whole[0].shape[1], side
    tok, col, row = blocks_of(h, whole[0], chunks)
    out, *wholes = pl.pallas_call(
        functools.partial(forward_kernel, side, chunks, layer),
        grid=(chunks,),
        in_specs=[tok, col, col, row] + [VMEM] * 3,
        out_specs=[tok] + [HBM] * 3,
        out_shape=[jax.ShapeDtypeStruct(h.shape, BF)] + wholes_of(side, weights),
        scratch_shapes=[pltpu.VMEM((tokens, width), BF), pltpu.VMEM((tokens, width), F32)] + gather_sems(side),
        compiler_params=pltpu.CompilerParams(
            dimension_semantics=("arbitrary",), vmem_limit_bytes=VMEM_LIMIT, collective_id=number, has_side_effects=True
        ),
        cost_estimate=pl.CostEstimate(flops=6 * tokens * width * hidden, bytes_accessed=4 * tokens * width, transcendentals=tokens * hidden),
        name="forward",
    )(h, *whole, *weights)
    return out, wholes


def chunk_terms(a_ref, dy_ref, wg_ref, wu_ref, wd_ref, sg, su, sd, total):
    for s in (sg, su, sd):
        s[...] = jnp.zeros_like(s)

    def main(rows):
        a, dy = a_ref[rows, :], dy_ref[rows, :]
        gate = dot(a, wg_ref[...])
        up = dot(a, wu_ref[...])
        dact = dot(dy, wd_ref[...], 1, 1).astype(BF).astype(F32)
        sig = jax.nn.sigmoid(gate)
        silu = gate * sig
        act = (silu * up).astype(BF)
        dup = (dact * silu).astype(BF)
        dgate = (dact * up * (sig + silu * (1 - sig))).astype(BF)
        sd[...] += dot(act, dy, 0, 0)
        sg[...] += dot(a, dgate, 0, 0)
        su[...] += dot(a, dup, 0, 0)
        if total is not None:
            total[rows, :] += dot(dgate, wg_ref[...], 1, 1) + dot(dup, wu_ref[...], 1, 1)

    over(a_ref.shape[0], 256, 2, main)


def carry_kernel(chunks, h_ref, dy_ref, wg_ref, wu_ref, wd_ref, dh_ref, gg_ref, gu_ref, gd_ref, a_ref, sg, su, sd, total):
    c = pl.program_id(0)
    pl.when(c == 0)(lambda: prepare(h_ref, a_ref, total))
    chunk_terms(a_ref, dy_ref, wg_ref, wu_ref, wd_ref, sg, su, sd, total)
    gd_ref[...] = sd[...].astype(BF)
    gg_ref[...] = sg[...].astype(BF)
    gu_ref[...] = su[...].astype(BF)

    @pl.when(c == chunks - 1)
    def _():
        def last(rows):
            wide = h_ref[rows, :].astype(F32)
            scale = scale_of(wide)
            da = total[rows, :].astype(BF).astype(F32)
            dwide = scale * (da - wide * (scale * scale * jnp.mean(da * wide, -1, keepdims=True)))
            dh_ref[rows, :] = dy_ref[rows, :] + dwide.astype(BF)

        over(h_ref.shape[0], 256, 1, last)


def sums_of(wg, wd, chunks):
    (width, hidden), chunk = wg.shape, wg.shape[1] // chunks
    return [pltpu.VMEM((width, chunk), F32), pltpu.VMEM((width, chunk), F32), pltpu.VMEM((chunk, width), F32)]


def backward_carry(side, h, dy, whole):
    (tokens, width), hidden, chunks = h.shape, whole[0].shape[1], side
    tok, col, row = blocks_of(h, whole[0], chunks)
    dh, *terms = pl.pallas_call(
        functools.partial(carry_kernel, chunks),
        grid=(chunks,),
        in_specs=[tok, tok, col, col, row],
        out_specs=[tok, col, col, row],
        out_shape=[jax.ShapeDtypeStruct(h.shape, BF)] + [jax.ShapeDtypeStruct(w.shape, BF) for w in whole],
        scratch_shapes=[pltpu.VMEM((tokens, width), BF), *sums_of(whole[0], whole[2], chunks), pltpu.VMEM((tokens, width), F32)],
        compiler_params=pltpu.CompilerParams(dimension_semantics=("arbitrary",), vmem_limit_bytes=VMEM_LIMIT),
        cost_estimate=pl.CostEstimate(flops=16 * tokens * width * hidden, bytes_accessed=6 * tokens * width, transcendentals=tokens * hidden),
        name="backward_carry",
    )(h, dy, *whole)
    return dh, terms


def last_kernel(side, chunks, h_ref, dy_ref, wg_ref, wu_ref, wd_ref, *rest):
    later, outs, outs_later, (a_ref, sg, su, sd), mine, (send_sems, recv_sems), scratch = (
        rest[0:3], rest[3:6], rest[6:9], rest[9:13], rest[13:16], rest[16:18], rest[18:]
    )
    half = len(scratch) // 2
    c = pl.program_id(0)
    place = Place(side, send_sems, recv_sems)
    above = Scattering(place, later, outs_later, scratch[:half], 1, 0, False)
    here = Scattering(place, mine, outs, scratch[half:], chunks, Scattering.copies(side, 1), True)
    parts = range(4)

    @pl.when(c == 0)
    def _():
        place.greet(False)
        for part in parts:
            above.send(part)
        prepare(h_ref, a_ref, None)

    @pl.when(c == chunks // 2)
    def _():
        for part in parts:
            above.add(part)

    @pl.when(c == chunks - 1)
    def _():
        for part in parts:
            above.finish(part)

    chunk_terms(a_ref, dy_ref, wg_ref, wu_ref, wd_ref, sg, su, sd, None)
    block = (side, side, mine[0].shape[2], sg.shape[1])
    mine[0][:, :, :, span(c, sg.shape[1])] = sg[...].astype(BF).reshape(block)
    mine[1][:, :, :, span(c, sg.shape[1])] = su[...].astype(BF).reshape(block)
    mine[2][c] = sd[...].astype(BF).reshape(mine[2].shape[1:])
    here.send(0, c)
    here.send(1, c)

    @pl.when(c == chunks - 1)
    def _():
        here.send(2)
        here.send(3)
        for part in parts:
            here.add(part)
        for part in parts:
            here.finish(part)


def backward_last(side, h, dy, whole, later, number):
    (tokens, width), hidden, chunks = h.shape, whole[0].shape[1], side
    tok, col, row = blocks_of(h, whole[0], chunks)
    shapes = [(t.shape[0] // side**2, t.shape[1]) for t in later]
    views = [(side, side, *s) for s in shapes]
    copies = Scattering.copies(side, 1) + Scattering.copies(side, chunks)
    found = pl.pallas_call(
        functools.partial(last_kernel, side, chunks),
        grid=(chunks,),
        in_specs=[tok, tok, col, col, row] + [HBM] * 3,
        out_specs=[VMEM] * 6,
        out_shape=[jax.ShapeDtypeStruct(s, BF) for s in shapes + shapes],
        scratch_shapes=[
            pltpu.VMEM((tokens, width), BF),
            *sums_of(whole[0], whole[2], chunks),
            *(pltpu.VMEM(v, BF) for v in views),
            DMA((copies,)),
            DMA((copies,)),
            *Scattering.scratch(side, shapes),
            *Scattering.scratch(side, shapes),
        ],
        compiler_params=pltpu.CompilerParams(
            dimension_semantics=("arbitrary",), vmem_limit_bytes=VMEM_LIMIT, collective_id=number, has_side_effects=True
        ),
        cost_estimate=pl.CostEstimate(flops=12 * tokens * width * hidden, bytes_accessed=4 * tokens * width, transcendentals=tokens * hidden),
        name="backward_last",
    )(h, dy, *whole, *(t.reshape(v) for t, v in zip(later, views, strict=True)))
    return found[:3], found[3:]


def adamw(w, m, v, g):
    m = 0.9 * m + 0.1 * g
    v = 0.95 * v + 0.05 * g * g
    step = m * lax.rsqrt(v + 1e-8) + 0.1 * w
    return (w - 0.02 * step).astype(BF), m, v


def solution(mesh):
    side = math.isqrt(mesh.shape["dp"])

    def step(x, dy, *arrays):
        weights, m, v = (arrays[i : i + 3] for i in (0, 3, 6))
        h = x[0]
        flat = lambda wholes: [w.reshape(-1, w.shape[-1]) for w in wholes]
        low = flat(gather(side, 0, weights, 1))
        above, high = forward(side, h, low, weights, 1, 2)
        dh, terms = backward_carry(side, above, dy[0], flat(high))
        mine = backward_last(side, h, dh, low, terms, 3)
        gradients = [jnp.stack([mine[number][i] for number in range(2)]).astype(F32) for i in range(3)]
        new = [adamw(w.astype(F32), m, v, g) for w, m, v, g in zip(weights, m, v, gradients, strict=True)]
        return tuple(one[which] for which in range(3) for one in new)

    states, cut = P(("rep", "dp"), None, None), P(None, "dp", None)
    return jax.shard_map(
        step,
        mesh=mesh,
        in_specs=(states, states) + (cut,) * 9,
        out_specs=(P("rep", "dp", None),) * 9,
        check_vma=False,
    )
```

```python
import functools
import math

import jax
import jax.numpy as jnp
from jax import lax
from jax.experimental import pallas as pl
from jax.experimental.pallas import tpu as pltpu
from jax.sharding import PartitionSpec as P

BF, F32 = jnp.bfloat16, jnp.float32
VMEM_LIMIT = 63 * 2**20
MESH = pl.DeviceIdType.MESH
HBM = pl.BlockSpec(memory_space=pltpu.HBM)
VMEM = pl.BlockSpec(memory_space=pltpu.VMEM)
DMA = pltpu.SemaphoreType.DMA


class Place:
    def __init__(self, side, send_sems, recv_sems):
        self.side, self.send_sems, self.recv_sems = side, send_sems, recv_sems
        me, rep = lax.axis_index("dp"), lax.axis_index("rep")
        self.at = (lax.div(me, side), lax.rem(me, side))
        self.parity = lax.rem(rep, 2)
        self.partner = {"rep": rep + 1 - 2 * self.parity}

    def along(self, axis, step):
        return lax.rem(self.at[axis] + step + self.side, self.side)

    def peer(self, axis, step):
        there = self.along(axis, step)
        return {"dp": there * self.side + self.at[1] if axis == 0 else self.at[0] * self.side + there}

    def greet(self, partner):
        barrier = pltpu.get_barrier_semaphore()
        peers = [self.peer(axis, step) for axis in (0, 1) for step in range(1, self.side)]
        peers += [self.partner] if partner else []
        for peer in peers:
            pl.semaphore_signal(barrier, inc=1, device_id=peer, device_id_type=MESH)
        pl.semaphore_wait(barrier, len(peers))

    def copy(self, number, src, dst, device):
        return pltpu.make_async_remote_copy(
            src_ref=src, dst_ref=dst, send_sem=self.send_sems.at[number], recv_sem=self.recv_sems.at[number], device_id=device, device_id_type=MESH
        )


def span(start, size):
    return pl.ds(pl.multiple_of(start * size, size), size)


class Gathering:
    @staticmethod
    def copies(side, parts, matrices):
        return parts * (side * side - 1) + matrices

    def __init__(self, place, items, local_sems, base=0):
        self.place, self.items, self.local_sems, self.base = place, items, local_sems, base

    def made(self):
        place, side, parity = self.place, self.place.side, self.place.parity
        parts = []
        last = []
        for block, whole, axis in self.items:
            half = block.shape[0] // 2
            if axis is None:
                parts += [(one, block, whole, span(2 * parity + one, half // 2)) for one in (0, 1)]
            else:
                parts.append((axis, block, whole, span(parity, half)))
            last.append(len(parts) - 1)

        def spot(whole, axis, behind, rows):
            a, b = place.along(axis, -behind), place.at[1 - axis]
            return whole.at[a, b, rows] if axis == 0 else whole.at[b, a, rows]

        kept, near, far, handed, number = [], {}, {}, {}, self.base
        for n, (axis, block, whole, rows) in enumerate(parts):
            src, own = block.at[rows], spot(whole, axis, 0, rows)
            kept.append(pltpu.make_async_copy(src, own, self.local_sems.at[n]))
            for step in range(1, side):
                near[n, step] = place.copy(number, src, own, place.peer(axis, step))
                far[n, step] = place.copy(number + 1, src, own, place.peer(1 - axis, step))
                number += 2
                here = spot(whole, axis, step, rows)
                for other in range(1, side):
                    handed[n, step, other] = place.copy(number, here, here, place.peer(1 - axis, other))
                    number += 1
        across = {}
        for n, (block, whole, _) in zip(last, self.items, strict=True):
            mine = whole.at[:, :, span(parity, block.shape[0] // 2)]
            across[n] = place.copy(number, mine, mine, place.partner)
            number += 1
        return kept, near, far, handed, across

    def send(self):
        kept, near, far, _, _ = self.made()
        for copy in kept:
            copy.start()
        for step in range(1, self.place.side):
            for n in range(len(kept)):
                near[n, step].start()
                far[n, step].start()

    def hand_on(self):
        kept, near, _, handed, _ = self.made()
        for step in range(1, self.place.side):
            for n in range(len(kept)):
                near[n, step].wait_recv()
                for other in range(1, self.place.side):
                    handed[n, step, other].start()

    def swap(self):
        kept, _, far, handed, across = self.made()
        for n, copy in enumerate(kept):
            copy.wait()
            for (part, *_), other in [*far.items(), *handed.items()]:
                if part == n:
                    other.wait_recv()
            if n in across:
                across[n].start()

    def finish(self):
        _, near, far, handed, across = self.made()
        for copy in [*near.values(), *far.values(), *handed.values()]:
            copy.wait_send()
        for copy in across.values():
            copy.wait_send()
            copy.wait_recv()


def gather_kernel(side, layer, g, u, g_whole, u_whole, send_sems, recv_sems, local_sems):
    place = Place(side, send_sems, recv_sems)
    run = Gathering(place, [(g.at[layer], g_whole, 0), (u.at[layer], u_whole, 1)], local_sems)
    place.greet(True)
    run.send()
    run.hand_on()
    run.swap()
    run.finish()


def wholes_of(side, weights):
    return [jax.ShapeDtypeStruct((side, side, *w.shape[1:]), w.dtype) for w in weights]


def gather(side, layer, weights, number):
    copies = Gathering.copies(side, 2, 2)
    return pl.pallas_call(
        functools.partial(gather_kernel, side, layer),
        in_specs=[VMEM] * 2,
        out_specs=[HBM] * 2,
        out_shape=wholes_of(side, weights),
        scratch_shapes=[DMA((copies,)), DMA((copies,)), DMA((2,))],
        compiler_params=pltpu.CompilerParams(collective_id=number, has_side_effects=True),
        name=f"gather_{number}",
    )(*weights)


class Scattering:
    @staticmethod
    def parts(shapes):
        (rows, columns), (middle, _), (tall, narrow) = shapes
        half = middle // 2
        return [(0, 0, 0, rows, columns), (0, 1, 0, half, columns), (1, 1, half, half, columns), (1, 2, 0, tall, narrow)]

    @staticmethod
    def copies(side, pieces):
        return (side - 1) * 8 * pieces

    @classmethod
    def scratch(cls, side, shapes):
        scratch = []
        for _, _, _, rows, columns in cls.parts(shapes):
            scratch += [pltpu.VMEM((side, side, rows, columns), BF), pltpu.VMEM((side, rows, columns), BF), pltpu.VMEM((side - 1, rows, columns), BF)]
        return scratch + [DMA((4,))]

    def __init__(self, place, terms, outs, scratch, pieces, base, local):
        self.place, self.terms, self.outs, self.pieces, self.base, self.local = place, terms, outs, pieces, base, local
        self.split = self.parts([out.shape for out in outs])
        self.first, self.partial, self.second, self.local_sems = scratch[0:12:3], scratch[1:12:3], scratch[2:12:3], scratch[12]

    def tall(self, part):
        return self.split[part][1] == 2

    def columns(self, part, piece):
        width = self.split[part][4]
        return pl.ds(0, width) if self.tall(part) else span(piece, width // self.pieces)

    def line(self, part, step, columns, piece):
        axis, matrix, start, rows, _ = self.split[part]
        there, within = self.place.along(axis, step), pl.ds(start, rows)
        if axis == 0:
            return self.terms[matrix].at[there, :, within, columns]
        return self.terms[matrix].at[slice(None) if piece is None else piece, there, within, columns]

    def near(self, part, piece):
        steps, columns = self.place.side - 1, self.columns(part, piece)
        number, which = self.base + steps * (part * self.pieces + piece), piece if self.tall(part) and self.pieces > 1 else None
        axis, copies = self.split[part][0], []
        for step in range(1, steps + 1):
            first = self.first[part].at[step, :, :, columns] if which is None else self.first[part].at[step, which]
            copies.append(self.place.copy(number + step - 1, self.line(part, step, columns, which), first, self.place.peer(axis, step)))
        return copies

    def own(self, part):
        return pltpu.make_async_copy(self.line(part, 0, self.columns(part, 0), None), self.first[part].at[0], self.local_sems.at[part])

    def far(self, part, piece):
        steps, axis, columns = self.place.side - 1, self.split[part][0], self.columns(part, piece)
        number = self.base + steps * (4 * self.pieces + part * self.pieces + piece)
        return [
            self.place.copy(
                number + step - 1,
                self.partial[part].at[self.place.along(1 - axis, step), :, columns],
                self.second[part].at[step - 1, :, columns],
                self.place.peer(1 - axis, step),
            )
            for step in range(1, steps + 1)
        ]

    def far_pieces(self, part):
        return [self.pieces - 1] if self.tall(part) else range(self.pieces)

    def send(self, part, piece=0):
        if not self.local:
            self.own(part).start()
        for copy in self.near(part, piece):
            copy.start()

    def add(self, part, piece=0):
        axis, matrix, start, rows, _ = self.split[part]
        first, partial, side = self.first[part], self.partial[part], self.place.side
        here, within, columns = self.place.at[axis], pl.ds(start, rows), self.columns(part, piece)
        if not self.local:
            self.own(part).wait()
        for copy in self.near(part, piece):
            copy.wait_recv()

        def one(k, _):
            if not self.local:
                total = first[0, k, :, columns].astype(F32)
            else:
                total = (self.terms[matrix][here, k, within, columns] if axis == 0 else self.terms[matrix][k, here, within, columns]).astype(F32)
            for step in range(1, side):
                total += first[step, k, :, columns].astype(F32)
            partial[k, :, columns] = total.astype(BF)
            return 0

        if self.tall(part) and self.pieces > 1:
            one(piece, 0)
        else:
            lax.fori_loop(0, side, one, 0)
        if piece in self.far_pieces(part):
            for copy in self.far(part, piece):
                copy.start()

    def finish(self, part):
        axis, matrix, start, rows, _ = self.split[part]
        for piece in self.far_pieces(part):
            for copy in self.far(part, piece):
                copy.wait_recv()
        total = self.partial[part][self.place.at[1 - axis]].astype(F32)
        for step in range(self.place.side - 1):
            total += self.second[part][step].astype(F32)
        self.outs[matrix][pl.ds(start, rows), :] = total.astype(BF)
        for piece in range(self.pieces):
            for copy in self.near(part, piece):
                copy.wait_send()
        for piece in self.far_pieces(part):
            for copy in self.far(part, piece):
                copy.wait_send()


def dot(a, b, ca=1, cb=0):
    return lax.dot_general(a, b, (((ca,), (cb,)), ((), ())), preferred_element_type=F32)


def scale_of(wide):
    return lax.rsqrt(jnp.mean(wide * wide, -1, keepdims=True) + 1e-6)


def over(tokens, tile, unroll, body):
    def step(t, _):
        body(span(t, tile))
        return 0

    lax.fori_loop(0, tokens // tile, step, 0, unroll=unroll)


def prepare(h_ref, a_ref, total):
    def first(rows):
        wide = h_ref[rows, :].astype(F32)
        a_ref[rows, :] = (wide * scale_of(wide)).astype(BF)
        if total is not None:
            total[rows, :] = jnp.zeros((rows.size, total.shape[1]), F32)

    over(h_ref.shape[0], 256, 1, first)


def forward_kernel(side, chunks, layer, h_ref, wg_ref, wu_ref, g, u, d, out_ref, *rest):
    low_whole, g_whole, u_whole, d_whole, a_ref, act_ref, wd_ref, send_sems, recv_sems, local_sems, load_sem = rest
    c = pl.program_id(0)
    place = Place(side, send_sems, recv_sems)
    low = Gathering(place, [(d.at[layer - 1], low_whole, None)], local_sems.at[0])
    high = Gathering(
        place,
        [(g.at[layer], g_whole, 0), (u.at[layer], u_whole, 1), (d.at[layer], d_whole, None)],
        local_sems.at[1],
        Gathering.copies(side, 2, 1),
    )
    load = pltpu.make_async_copy(low_whole, wd_ref, load_sem)

    @pl.when(c == 0)
    def _():
        place.greet(True)
        low.send()
        high.send()
        prepare(h_ref, a_ref, None)

    @pl.when(c == 1)
    def _():
        low.hand_on()
        high.hand_on()

    pl.when(c == chunks - 2)(low.swap)

    @pl.when(c == chunks - 1)
    def _():
        low.finish()
        load.start()
        high.swap()

    def main(rows):
        a = a_ref[rows, :]
        gate = dot(a, wg_ref[...])
        up = dot(a, wu_ref[...])
        act_ref[rows, span(c, wg_ref.shape[1])] = (gate * jax.nn.sigmoid(gate) * up).astype(BF)

    over(h_ref.shape[0], 512, 1, main)

    @pl.when(c == chunks - 1)
    def _():
        load.wait()

        def last(rows):
            wd = wd_ref[...].reshape(act_ref.shape[1], h_ref.shape[1])
            out_ref[rows, :] = h_ref[rows, :] + dot(act_ref[rows, :], wd).astype(BF)

        over(h_ref.shape[0], 512, 1, last)
        high.finish()


def blocks_of(h, wg, chunks):
    tokens, width = h.shape
    chunk = wg.shape[1] // chunks
    tok = pl.BlockSpec((tokens, width), lambda c: (0, 0), pipeline_mode=pl.Buffered(1))
    return tok, pl.BlockSpec((width, chunk), lambda c: (0, c)), pl.BlockSpec((chunk, width), lambda c: (c, 0))


def forward(side, h, whole, weights, layer, number):
    (tokens, width), hidden, chunks = h.shape, whole[0].shape[1], side
    tok, col, row = blocks_of(h, whole[0], chunks)
    down, *_ = wholes_of(side, weights[2:])
    copies = Gathering.copies(side, 2, 1) + Gathering.copies(side, 4, 3)
    out, *wholes = pl.pallas_call(
        functools.partial(forward_kernel, side, chunks, layer),
        grid=(chunks,),
        in_specs=[tok, col, col] + [VMEM] * 3,
        out_specs=[tok] + [HBM] * 4,
        out_shape=[jax.ShapeDtypeStruct(h.shape, BF), down] + wholes_of(side, weights),
        scratch_shapes=[
            pltpu.VMEM((tokens, width), BF),
            pltpu.VMEM((tokens, hidden), BF),
            pltpu.VMEM(down.shape, BF),
            DMA((copies,)),
            DMA((copies,)),
            DMA((2, 4)),
            DMA(()),
        ],
        compiler_params=pltpu.CompilerParams(
            dimension_semantics=("arbitrary",), vmem_limit_bytes=VMEM_LIMIT, collective_id=number, has_side_effects=True
        ),
        cost_estimate=pl.CostEstimate(flops=6 * tokens * width * hidden, bytes_accessed=4 * tokens * width, transcendentals=tokens * hidden),
        name="forward",
    )(h, *whole, *weights)
    return out, wholes[0], wholes[1:]


def chunk_terms(a_ref, dy_ref, wg_ref, wu_ref, wd_ref, sg, su, sd, total):
    for s in (sg, su, sd):
        s[...] = jnp.zeros_like(s)

    def main(rows):
        a, dy = a_ref[rows, :], dy_ref[rows, :]
        gate = dot(a, wg_ref[...])
        up = dot(a, wu_ref[...])
        dact = dot(dy, wd_ref[...], 1, 1).astype(BF).astype(F32)
        sig = jax.nn.sigmoid(gate)
        silu = gate * sig
        act = (silu * up).astype(BF)
        dup = (dact * silu).astype(BF)
        dgate = (dact * up * (sig + silu * (1 - sig))).astype(BF)
        sd[...] += dot(act, dy, 0, 0)
        sg[...] += dot(a, dgate, 0, 0)
        su[...] += dot(a, dup, 0, 0)
        if total is not None:
            total[rows, :] += dot(dgate, wg_ref[...], 1, 1) + dot(dup, wu_ref[...], 1, 1)

    over(a_ref.shape[0], 256, 2, main)


def carry_kernel(chunks, h_ref, dy_ref, wg_ref, wu_ref, wd_ref, dh_ref, gg_ref, gu_ref, gd_ref, a_ref, sg, su, sd, total):
    c = pl.program_id(0)
    pl.when(c == 0)(lambda: prepare(h_ref, a_ref, total))
    chunk_terms(a_ref, dy_ref, wg_ref, wu_ref, wd_ref, sg, su, sd, total)
    gd_ref[...] = sd[...].astype(BF)
    gg_ref[...] = sg[...].astype(BF)
    gu_ref[...] = su[...].astype(BF)

    @pl.when(c == chunks - 1)
    def _():
        def last(rows):
            wide = h_ref[rows, :].astype(F32)
            scale = scale_of(wide)
            da = total[rows, :].astype(BF).astype(F32)
            dwide = scale * (da - wide * (scale * scale * jnp.mean(da * wide, -1, keepdims=True)))
            dh_ref[rows, :] = dy_ref[rows, :] + dwide.astype(BF)

        over(h_ref.shape[0], 256, 1, last)


def sums_of(wg, wd, chunks):
    (width, hidden), chunk = wg.shape, wg.shape[1] // chunks
    return [pltpu.VMEM((width, chunk), F32), pltpu.VMEM((width, chunk), F32), pltpu.VMEM((chunk, width), F32)]


def backward_carry(side, h, dy, whole):
    (tokens, width), hidden, chunks = h.shape, whole[0].shape[1], side
    tok, col, row = blocks_of(h, whole[0], chunks)
    dh, *terms = pl.pallas_call(
        functools.partial(carry_kernel, chunks),
        grid=(chunks,),
        in_specs=[tok, tok, col, col, row],
        out_specs=[tok, col, col, row],
        out_shape=[jax.ShapeDtypeStruct(h.shape, BF)] + [jax.ShapeDtypeStruct(w.shape, BF) for w in whole],
        scratch_shapes=[pltpu.VMEM((tokens, width), BF), *sums_of(whole[0], whole[2], chunks), pltpu.VMEM((tokens, width), F32)],
        compiler_params=pltpu.CompilerParams(dimension_semantics=("arbitrary",), vmem_limit_bytes=VMEM_LIMIT),
        cost_estimate=pl.CostEstimate(flops=16 * tokens * width * hidden, bytes_accessed=6 * tokens * width, transcendentals=tokens * hidden),
        name="backward_carry",
    )(h, dy, *whole)
    return dh, terms


def last_kernel(side, chunks, h_ref, dy_ref, wg_ref, wu_ref, wd_ref, *rest):
    later, outs, outs_later, (a_ref, sg, su, sd), mine, (send_sems, recv_sems), scratch = (
        rest[0:3], rest[3:6], rest[6:9], rest[9:13], rest[13:16], rest[16:18], rest[18:]
    )
    half = len(scratch) // 2
    c = pl.program_id(0)
    place = Place(side, send_sems, recv_sems)
    above = Scattering(place, later, outs_later, scratch[:half], 1, 0, False)
    here = Scattering(place, mine, outs, scratch[half:], chunks, Scattering.copies(side, 1), True)
    parts = range(4)

    @pl.when(c == 0)
    def _():
        place.greet(False)
        for part in parts:
            above.send(part)
        prepare(h_ref, a_ref, None)

    @pl.when(c == chunks // 2)
    def _():
        for part in parts:
            above.add(part)

    @pl.when(c == chunks - 1)
    def _():
        for part in parts:
            above.finish(part)
        for piece in range(chunks - 2):
            for part in parts:
                here.add(part, piece)

    chunk_terms(a_ref, dy_ref, wg_ref, wu_ref, wd_ref, sg, su, sd, None)
    block = (side, side, mine[0].shape[2], sg.shape[1])
    mine[0][:, :, :, span(c, sg.shape[1])] = sg[...].astype(BF).reshape(block)
    mine[1][:, :, :, span(c, sg.shape[1])] = su[...].astype(BF).reshape(block)
    mine[2][c] = sd[...].astype(BF).reshape(mine[2].shape[1:])
    for part in parts:
        here.send(part, c)

    @pl.when(c == chunks - 1)
    def _():
        for piece in range(chunks - 2, chunks):
            for part in parts:
                here.add(part, piece)
        for part in parts:
            here.finish(part)


def backward_last(side, h, dy, whole, later, number):
    (tokens, width), hidden, chunks = h.shape, whole[0].shape[1], side
    tok, col, row = blocks_of(h, whole[0], chunks)
    shapes = [(t.shape[0] // side**2, t.shape[1]) for t in later]
    views = [(side, side, *s) for s in shapes]
    copies = Scattering.copies(side, 1) + Scattering.copies(side, chunks)
    found = pl.pallas_call(
        functools.partial(last_kernel, side, chunks),
        grid=(chunks,),
        in_specs=[tok, tok, col, col, row] + [HBM] * 3,
        out_specs=[VMEM] * 6,
        out_shape=[jax.ShapeDtypeStruct(s, BF) for s in shapes + shapes],
        scratch_shapes=[
            pltpu.VMEM((tokens, width), BF),
            *sums_of(whole[0], whole[2], chunks),
            *(pltpu.VMEM(v, BF) for v in views),
            DMA((copies,)),
            DMA((copies,)),
            *Scattering.scratch(side, shapes),
            *Scattering.scratch(side, shapes),
        ],
        compiler_params=pltpu.CompilerParams(
            dimension_semantics=("arbitrary",), vmem_limit_bytes=VMEM_LIMIT, collective_id=number, has_side_effects=True
        ),
        cost_estimate=pl.CostEstimate(flops=12 * tokens * width * hidden, bytes_accessed=4 * tokens * width, transcendentals=tokens * hidden),
        name="backward_last",
    )(h, dy, *whole, *(t.reshape(v) for t, v in zip(later, views, strict=True)))
    return found[:3], found[3:]


def adamw(w, m, v, g):
    m = 0.9 * m + 0.1 * g
    v = 0.95 * v + 0.05 * g * g
    step = m * lax.rsqrt(v + 1e-8) + 0.1 * w
    return (w - 0.02 * step).astype(BF), m, v


def solution(mesh):
    side = math.isqrt(mesh.shape["dp"])

    def step(x, dy, *arrays):
        weights, m, v = (arrays[i : i + 3] for i in (0, 3, 6))
        h = x[0]
        flat = lambda wholes: [w.reshape(-1, w.shape[-1]) for w in wholes]
        low = flat(gather(side, 0, weights[:2], 1))
        above, down, high = forward(side, h, low, weights, 1, 2)
        low += flat([down])
        dh, terms = backward_carry(side, above, dy[0], flat(high))
        mine = backward_last(side, h, dh, low, terms, 3)
        gradients = [jnp.stack([mine[number][i] for number in range(2)]).astype(F32) for i in range(3)]
        new = [adamw(w.astype(F32), m, v, g) for w, m, v, g in zip(weights, m, v, gradients, strict=True)]
        return tuple(one[which] for which in range(3) for one in new)

    states, cut = P(("rep", "dp"), None, None), P(None, "dp", None)
    return jax.shard_map(
        step,
        mesh=mesh,
        in_specs=(states, states) + (cut,) * 9,
        out_specs=(P("rep", "dp", None),) * 9,
        check_vma=False,
    )
```

```python
import functools
import math

import jax
import jax.numpy as jnp
from jax import lax
from jax.experimental import pallas as pl
from jax.experimental.pallas import tpu as pltpu
from jax.sharding import PartitionSpec as P

BF, F32 = jnp.bfloat16, jnp.float32
VMEM_LIMIT = 63 * 2**20
MESH = pl.DeviceIdType.MESH
HBM = pl.BlockSpec(memory_space=pltpu.HBM)
VMEM = pl.BlockSpec(memory_space=pltpu.VMEM)
DMA = pltpu.SemaphoreType.DMA


class Place:
    def __init__(self, side, send_sems, recv_sems):
        self.side, self.send_sems, self.recv_sems = side, send_sems, recv_sems
        me, rep = lax.axis_index("dp"), lax.axis_index("rep")
        self.at = (lax.div(me, side), lax.rem(me, side))
        self.parity = lax.rem(rep, 2)
        self.partner = {"rep": rep + 1 - 2 * self.parity}

    def along(self, axis, step):
        return lax.rem(self.at[axis] + step + self.side, self.side)

    def peer(self, axis, step):
        there = self.along(axis, step)
        return {"dp": there * self.side + self.at[1] if axis == 0 else self.at[0] * self.side + there}

    def greet(self, partner):
        barrier = pltpu.get_barrier_semaphore()
        peers = [self.peer(axis, step) for axis in (0, 1) for step in range(1, self.side)]
        peers += [self.partner] if partner else []
        for peer in peers:
            pl.semaphore_signal(barrier, inc=1, device_id=peer, device_id_type=MESH)
        pl.semaphore_wait(barrier, len(peers))

    def copy(self, number, src, dst, device):
        return pltpu.make_async_remote_copy(
            src_ref=src, dst_ref=dst, send_sem=self.send_sems.at[number], recv_sem=self.recv_sems.at[number], device_id=device, device_id_type=MESH
        )


def span(start, size):
    return pl.ds(pl.multiple_of(start * size, size), size)


class Gathering:
    @staticmethod
    def copies(side, parts, matrices):
        return parts * (side * side - 1) + matrices

    def __init__(self, place, items, local_sems, base=0):
        self.place, self.items, self.local_sems, self.base = place, items, local_sems, base

    def made(self):
        place, side, parity = self.place, self.place.side, self.place.parity
        parts = []
        last = []
        for block, whole, axis in self.items:
            half = block.shape[0] // 2
            if axis is None:
                parts += [(one, block, whole, span(2 * parity + one, half // 2)) for one in (0, 1)]
            else:
                parts.append((axis, block, whole, span(parity, half)))
            last.append(len(parts) - 1)

        def spot(whole, axis, behind, rows):
            a, b = place.along(axis, -behind), place.at[1 - axis]
            return whole.at[a, b, rows] if axis == 0 else whole.at[b, a, rows]

        kept, near, far, handed, number = [], {}, {}, {}, self.base
        for n, (axis, block, whole, rows) in enumerate(parts):
            src, own = block.at[rows], spot(whole, axis, 0, rows)
            kept.append(pltpu.make_async_copy(src, own, self.local_sems.at[n]))
            for step in range(1, side):
                near[n, step] = place.copy(number, src, own, place.peer(axis, step))
                far[n, step] = place.copy(number + 1, src, own, place.peer(1 - axis, step))
                number += 2
                here = spot(whole, axis, step, rows)
                for other in range(1, side):
                    handed[n, step, other] = place.copy(number, here, here, place.peer(1 - axis, other))
                    number += 1
        across = {}
        for n, (block, whole, _) in zip(last, self.items, strict=True):
            mine = whole.at[:, :, span(parity, block.shape[0] // 2)]
            across[n] = place.copy(number, mine, mine, place.partner)
            number += 1
        return kept, near, far, handed, across

    def send(self):
        kept, near, far, _, _ = self.made()
        for copy in kept:
            copy.start()
        for step in range(1, self.place.side):
            for n in range(len(kept)):
                near[n, step].start()
                far[n, step].start()

    def hand_on(self):
        kept, near, _, handed, _ = self.made()
        for step in range(1, self.place.side):
            for n in range(len(kept)):
                near[n, step].wait_recv()
                for other in range(1, self.place.side):
                    handed[n, step, other].start()

    def swap(self):
        kept, _, far, handed, across = self.made()
        for n, copy in enumerate(kept):
            copy.wait()
            for (part, *_), other in [*far.items(), *handed.items()]:
                if part == n:
                    other.wait_recv()
            if n in across:
                across[n].start()

    def finish(self):
        _, near, far, handed, across = self.made()
        for copy in [*near.values(), *far.values(), *handed.values()]:
            copy.wait_send()
        for copy in across.values():
            copy.wait_send()
            copy.wait_recv()


def gather_kernel(side, layer, g, u, g_whole, u_whole, send_sems, recv_sems, local_sems):
    place = Place(side, send_sems, recv_sems)
    run = Gathering(place, [(g.at[layer], g_whole, 0), (u.at[layer], u_whole, 1)], local_sems)
    place.greet(True)
    run.send()
    run.hand_on()
    run.swap()
    run.finish()


def wholes_of(side, weights):
    return [jax.ShapeDtypeStruct((side, side, *w.shape[1:]), w.dtype) for w in weights]


def gather(side, layer, weights, number):
    copies = Gathering.copies(side, 2, 2)
    return pl.pallas_call(
        functools.partial(gather_kernel, side, layer),
        in_specs=[VMEM] * 2,
        out_specs=[HBM] * 2,
        out_shape=wholes_of(side, weights),
        scratch_shapes=[DMA((copies,)), DMA((copies,)), DMA((2,))],
        compiler_params=pltpu.CompilerParams(collective_id=number, has_side_effects=True),
        name=f"gather_{number}",
    )(*weights)


class Scattering:
    @staticmethod
    def parts(shapes):
        (rows, columns), (middle, _), (tall, narrow) = shapes
        half = middle // 2
        return [(0, 0, 0, rows, columns), (0, 1, 0, half, columns), (1, 1, half, half, columns), (1, 2, 0, tall, narrow)]

    @staticmethod
    def copies(side, pieces):
        return (side - 1) * 8 * pieces

    @classmethod
    def scratch(cls, side, shapes):
        scratch = []
        for _, _, _, rows, columns in cls.parts(shapes):
            scratch += [pltpu.VMEM((side, side, rows, columns), BF), pltpu.VMEM((side, rows, columns), BF), pltpu.VMEM((side - 1, rows, columns), BF)]
        return scratch + [DMA((4,))]

    def __init__(self, place, terms, outs, scratch, pieces, base, local, shapes):
        self.place, self.terms, self.outs, self.pieces, self.base, self.local = place, terms, outs, pieces, base, local
        self.split = self.parts(shapes)
        self.first, self.partial, self.second, self.local_sems = scratch[0:12:3], scratch[1:12:3], scratch[2:12:3], scratch[12]

    def tall(self, part):
        return self.split[part][1] == 2

    def columns(self, part, piece):
        width = self.split[part][4]
        return pl.ds(0, width) if self.tall(part) else span(piece, width // self.pieces)

    def line(self, part, step, columns, piece):
        axis, matrix, start, rows, _ = self.split[part]
        there, within = self.place.along(axis, step), pl.ds(start, rows)
        if axis == 0:
            return self.terms[matrix].at[there, :, within, columns]
        return self.terms[matrix].at[slice(None) if piece is None else piece, there, within, columns]

    def near(self, part, piece):
        steps, columns = self.place.side - 1, self.columns(part, piece)
        number, which = self.base + steps * (part * self.pieces + piece), piece if self.tall(part) and self.pieces > 1 else None
        axis, copies = self.split[part][0], []
        for step in range(1, steps + 1):
            first = self.first[part].at[step, :, :, columns] if which is None else self.first[part].at[step, which]
            copies.append(self.place.copy(number + step - 1, self.line(part, step, columns, which), first, self.place.peer(axis, step)))
        return copies

    def own(self, part):
        return pltpu.make_async_copy(self.line(part, 0, self.columns(part, 0), None), self.first[part].at[0], self.local_sems.at[part])

    def far(self, part, piece):
        steps, axis, columns = self.place.side - 1, self.split[part][0], self.columns(part, piece)
        number = self.base + steps * (4 * self.pieces + part * self.pieces + piece)
        return [
            self.place.copy(
                number + step - 1,
                self.partial[part].at[self.place.along(1 - axis, step), :, columns],
                self.second[part].at[step - 1, :, columns],
                self.place.peer(1 - axis, step),
            )
            for step in range(1, steps + 1)
        ]

    def far_pieces(self, part):
        return [self.pieces - 1] if self.tall(part) else range(self.pieces)

    def send(self, part, piece=0):
        if not self.local:
            self.own(part).start()
        for copy in self.near(part, piece):
            copy.start()

    def add(self, part, piece=0):
        axis, matrix, start, rows, _ = self.split[part]
        first, partial, side = self.first[part], self.partial[part], self.place.side
        here, within, columns = self.place.at[axis], pl.ds(start, rows), self.columns(part, piece)
        if not self.local:
            self.own(part).wait()
        for copy in self.near(part, piece):
            copy.wait_recv()

        def one(k, _):
            if not self.local:
                total = first[0, k, :, columns].astype(F32)
            else:
                total = (self.terms[matrix][here, k, within, columns] if axis == 0 else self.terms[matrix][k, here, within, columns]).astype(F32)
            for step in range(1, side):
                total += first[step, k, :, columns].astype(F32)
            partial[k, :, columns] = total.astype(BF)
            return 0

        if self.tall(part) and self.pieces > 1:
            one(piece, 0)
        else:
            lax.fori_loop(0, side, one, 0)
        if piece in self.far_pieces(part):
            for copy in self.far(part, piece):
                copy.start()

    def finish(self, part, pieces=None):
        axis, matrix, start, rows, _ = self.split[part]
        pieces = range(self.pieces if pieces is None else pieces)
        far = self.far_pieces(part) if self.tall(part) else pieces
        for piece in far:
            for copy in self.far(part, piece):
                copy.wait_recv()
            columns = self.columns(part, piece)
            total = self.partial[part][self.place.at[1 - axis], :, columns].astype(F32)
            for step in range(self.place.side - 1):
                total += self.second[part][step, :, columns].astype(F32)
            self.outs[matrix][pl.ds(start, rows), columns] = total.astype(BF)
        for piece in pieces:
            for copy in self.near(part, piece):
                copy.wait_send()
        for piece in far:
            for copy in self.far(part, piece):
                copy.wait_send()


def dot(a, b, ca=1, cb=0):
    return lax.dot_general(a, b, (((ca,), (cb,)), ((), ())), preferred_element_type=F32)


def scale_of(wide):
    return lax.rsqrt(jnp.mean(wide * wide, -1, keepdims=True) + 1e-6)


def over(tokens, tile, unroll, body):
    def step(t, _):
        body(span(t, tile))
        return 0

    lax.fori_loop(0, tokens // tile, step, 0, unroll=unroll)


def prepare(h_ref, a_ref, total):
    def first(rows):
        wide = h_ref[rows, :].astype(F32)
        a_ref[rows, :] = (wide * scale_of(wide)).astype(BF)
        if total is not None:
            total[rows, :] = jnp.zeros((rows.size, total.shape[1]), F32)

    over(h_ref.shape[0], 256, 1, first)


def forward_kernel(side, chunks, layer, h_ref, wg_ref, wu_ref, g, u, d, out_ref, *rest):
    low_whole, g_whole, u_whole, d_whole, a_ref, act_ref, wd_ref, send_sems, recv_sems, local_sems, load_sem = rest
    c = pl.program_id(0)
    place = Place(side, send_sems, recv_sems)
    low = Gathering(place, [(d.at[layer - 1], low_whole, None)], local_sems.at[0])
    high = Gathering(
        place,
        [(g.at[layer], g_whole, 0), (u.at[layer], u_whole, 1), (d.at[layer], d_whole, None)],
        local_sems.at[1],
        Gathering.copies(side, 2, 1),
    )
    load = pltpu.make_async_copy(low_whole, wd_ref, load_sem)

    @pl.when(c == 0)
    def _():
        place.greet(True)
        low.send()
        high.send()
        prepare(h_ref, a_ref, None)

    @pl.when(c == 1)
    def _():
        low.hand_on()
        high.hand_on()

    pl.when(c == chunks - 2)(low.swap)

    @pl.when(c == chunks - 1)
    def _():
        low.finish()
        load.start()

    def main(rows):
        a = a_ref[rows, :]
        gate = dot(a, wg_ref[...])
        up = dot(a, wu_ref[...])
        act_ref[rows, span(c, wg_ref.shape[1])] = (gate * jax.nn.sigmoid(gate) * up).astype(BF)

    over(h_ref.shape[0], 512, 1, main)

    @pl.when(c == chunks - 1)
    def _():
        load.wait()
        high.swap()

        def last(rows):
            wd = wd_ref[...].reshape(act_ref.shape[1], h_ref.shape[1])
            out_ref[rows, :] = h_ref[rows, :] + dot(act_ref[rows, :], wd).astype(BF)

        over(h_ref.shape[0], 512, 1, last)
        high.finish()


def blocks_of(h, wg, chunks):
    tokens, width = h.shape
    chunk = wg.shape[1] // chunks
    tok = pl.BlockSpec((tokens, width), lambda c: (0, 0), pipeline_mode=pl.Buffered(1))
    return tok, pl.BlockSpec((width, chunk), lambda c: (0, c)), pl.BlockSpec((chunk, width), lambda c: (c, 0))


def forward(side, h, whole, weights, layer, number):
    (tokens, width), hidden, chunks = h.shape, whole[0].shape[1], side
    tok, col, row = blocks_of(h, whole[0], chunks)
    down, *_ = wholes_of(side, weights[2:])
    copies = Gathering.copies(side, 2, 1) + Gathering.copies(side, 4, 3)
    out, *wholes = pl.pallas_call(
        functools.partial(forward_kernel, side, chunks, layer),
        grid=(chunks,),
        in_specs=[tok, col, col] + [VMEM] * 3,
        out_specs=[tok] + [HBM] * 4,
        out_shape=[jax.ShapeDtypeStruct(h.shape, BF), down] + wholes_of(side, weights),
        scratch_shapes=[
            pltpu.VMEM((tokens, width), BF),
            pltpu.VMEM((tokens, hidden), BF),
            pltpu.VMEM(down.shape, BF),
            DMA((copies,)),
            DMA((copies,)),
            DMA((2, 4)),
            DMA(()),
        ],
        compiler_params=pltpu.CompilerParams(
            dimension_semantics=("arbitrary",), vmem_limit_bytes=VMEM_LIMIT, collective_id=number, has_side_effects=True
        ),
        cost_estimate=pl.CostEstimate(flops=6 * tokens * width * hidden, bytes_accessed=4 * tokens * width, transcendentals=tokens * hidden),
        name="forward",
    )(h, *whole, *weights)
    return out, wholes[0], wholes[1:]


def chunk_terms(a_ref, dy_ref, wg_ref, wu_ref, wd_ref, sg, su, sd, total):
    for s in (sg, su, sd):
        s[...] = jnp.zeros_like(s)

    def main(rows):
        a, dy = a_ref[rows, :], dy_ref[rows, :]
        gate = dot(a, wg_ref[...])
        up = dot(a, wu_ref[...])
        dact = dot(dy, wd_ref[...], 1, 1).astype(BF).astype(F32)
        sig = jax.nn.sigmoid(gate)
        silu = gate * sig
        act = (silu * up).astype(BF)
        dup = (dact * silu).astype(BF)
        dgate = (dact * up * (sig + silu * (1 - sig))).astype(BF)
        sd[...] += dot(act, dy, 0, 0)
        sg[...] += dot(a, dgate, 0, 0)
        su[...] += dot(a, dup, 0, 0)
        if total is not None:
            total[rows, :] += dot(dgate, wg_ref[...], 1, 1) + dot(dup, wu_ref[...], 1, 1)

    over(a_ref.shape[0], 256, 2, main)


def carry_kernel(side, chunks, shapes, h_ref, dy_ref, wg_ref, wu_ref, wd_ref, dh_ref, gg_ref, gu_ref, gd_ref, eg_ref, eu_ref, *rest):
    (a_ref, sg, su, sd, total), mine, (send_sems, recv_sems), scratch = rest[:5], rest[5:7], rest[7:9], rest[9:]
    c = pl.program_id(0)
    place = Place(side, send_sems, recv_sems)
    early = Scattering(place, (*mine, None), (eg_ref, eu_ref, None), scratch, chunks, 0, True, shapes)
    parts = range(3)

    @pl.when(c == 0)
    def _():
        place.greet(False)
        prepare(h_ref, a_ref, total)

    for piece in range(chunks - 2):

        @pl.when(c == piece + 2)
        def _(piece=piece):
            for part in parts:
                early.add(part, piece)

    chunk_terms(a_ref, dy_ref, wg_ref, wu_ref, wd_ref, sg, su, sd, total)
    gd_ref[...] = sd[...].astype(BF)

    @pl.when(c < chunks - 1)
    def _():
        block = (side, side, mine[0].shape[2], sg.shape[1])
        mine[0][:, :, :, span(c, sg.shape[1])] = sg[...].astype(BF).reshape(block)
        mine[1][:, :, :, span(c, sg.shape[1])] = su[...].astype(BF).reshape(block)
        for part in parts:
            early.send(part, c)

    @pl.when(c == chunks - 1)
    def _():
        for part in parts:
            early.add(part, chunks - 2)
        gg_ref[...] = sg[...].astype(BF)
        gu_ref[...] = su[...].astype(BF)

        def last(rows):
            wide = h_ref[rows, :].astype(F32)
            scale = scale_of(wide)
            da = total[rows, :].astype(BF).astype(F32)
            dwide = scale * (da - wide * (scale * scale * jnp.mean(da * wide, -1, keepdims=True)))
            dh_ref[rows, :] = dy_ref[rows, :] + dwide.astype(BF)

        over(h_ref.shape[0], 256, 1, last)
        for part in parts:
            early.finish(part, chunks - 1)


def sums_of(wg, wd, chunks):
    (width, hidden), chunk = wg.shape, wg.shape[1] // chunks
    return [pltpu.VMEM((width, chunk), F32), pltpu.VMEM((width, chunk), F32), pltpu.VMEM((chunk, width), F32)]


def backward_carry(side, h, dy, whole, number):
    (tokens, width), hidden, chunks = h.shape, whole[0].shape[1], side
    chunk = hidden // chunks
    tok, col, row = blocks_of(h, whole[0], chunks)
    shapes = [(w.shape[0] // side**2, w.shape[1]) for w in whole]
    one = pl.BlockSpec((width, chunk), lambda c: (0, 0))
    copies = Scattering.copies(side, chunks)
    summed = (shapes[0][0], hidden - chunk)
    dh, gg, gu, gd, eg, eu = pl.pallas_call(
        functools.partial(carry_kernel, side, chunks, shapes),
        grid=(chunks,),
        in_specs=[tok, tok, col, col, row],
        out_specs=[tok, one, one, row, VMEM, VMEM],
        out_shape=[
            jax.ShapeDtypeStruct(h.shape, BF),
            *[jax.ShapeDtypeStruct((width, chunk), BF)] * 2,
            jax.ShapeDtypeStruct(whole[2].shape, BF),
            *[jax.ShapeDtypeStruct(summed, BF)] * 2,
        ],
        scratch_shapes=[
            pltpu.VMEM((tokens, width), BF),
            *sums_of(whole[0], whole[2], chunks),
            pltpu.VMEM((tokens, width), F32),
            *(pltpu.VMEM((side, side, *s), BF) for s in shapes[:2]),
            DMA((copies,)),
            DMA((copies,)),
            *Scattering.scratch(side, shapes),
        ],
        compiler_params=pltpu.CompilerParams(
            dimension_semantics=("arbitrary",), vmem_limit_bytes=VMEM_LIMIT, collective_id=number, has_side_effects=True
        ),
        cost_estimate=pl.CostEstimate(flops=16 * tokens * width * hidden, bytes_accessed=6 * tokens * width, transcendentals=tokens * hidden),
        name="backward_carry",
    )(h, dy, *whole)
    return dh, (gg, gu, gd), (eg, eu)


def last_kernel(side, chunks, shapes, late, h_ref, dy_ref, wg_ref, wu_ref, wd_ref, *rest):
    later, outs, outs_later, (a_ref, sg, su, sd), mine, (send_sems, recv_sems), scratch = (
        rest[0:3], rest[3:6], rest[6:9], rest[9:13], rest[13:16], rest[16:18], rest[18:]
    )
    half = len(scratch) // 2
    c = pl.program_id(0)
    place = Place(side, send_sems, recv_sems)
    above = Scattering(place, later, outs_later, scratch[:half], 1, 0, False, late)
    here = Scattering(place, mine, outs, scratch[half:], chunks, Scattering.copies(side, 1), True, shapes)
    parts = range(4)

    @pl.when(c == 0)
    def _():
        place.greet(False)
        for part in parts:
            above.send(part)
        prepare(h_ref, a_ref, None)

    @pl.when(c == chunks // 2)
    def _():
        for part in parts:
            above.add(part)

    @pl.when(c == chunks - 1)
    def _():
        for part in parts:
            above.finish(part)
        for piece in range(chunks - 2):
            for part in parts:
                here.add(part, piece)

    chunk_terms(a_ref, dy_ref, wg_ref, wu_ref, wd_ref, sg, su, sd, None)
    block = (side, side, mine[0].shape[2], sg.shape[1])
    mine[0][:, :, :, span(c, sg.shape[1])] = sg[...].astype(BF).reshape(block)
    mine[1][:, :, :, span(c, sg.shape[1])] = su[...].astype(BF).reshape(block)
    mine[2][c] = sd[...].astype(BF).reshape(mine[2].shape[1:])
    for part in parts:
        here.send(part, c)

    @pl.when(c == chunks - 1)
    def _():
        for piece in range(chunks - 2, chunks):
            for part in parts:
                here.add(part, piece)
        for part in parts:
            here.finish(part)


def backward_last(side, h, dy, whole, later, number):
    (tokens, width), hidden, chunks = h.shape, whole[0].shape[1], side
    tok, col, row = blocks_of(h, whole[0], chunks)
    late = [(t.shape[0] // side**2, t.shape[1]) for t in later]
    shapes = [(w.shape[0] // side**2, w.shape[1]) for w in whole]
    views = [(side, side, *s) for s in shapes]
    copies = Scattering.copies(side, 1) + Scattering.copies(side, chunks)
    found = pl.pallas_call(
        functools.partial(last_kernel, side, chunks, shapes, late),
        grid=(chunks,),
        in_specs=[tok, tok, col, col, row] + [HBM] * 3,
        out_specs=[VMEM] * 6,
        out_shape=[jax.ShapeDtypeStruct(s, BF) for s in shapes + late],
        scratch_shapes=[
            pltpu.VMEM((tokens, width), BF),
            *sums_of(whole[0], whole[2], chunks),
            *(pltpu.VMEM(v, BF) for v in views),
            DMA((copies,)),
            DMA((copies,)),
            *Scattering.scratch(side, late),
            *Scattering.scratch(side, shapes),
        ],
        compiler_params=pltpu.CompilerParams(
            dimension_semantics=("arbitrary",), vmem_limit_bytes=VMEM_LIMIT, collective_id=number, has_side_effects=True
        ),
        cost_estimate=pl.CostEstimate(flops=12 * tokens * width * hidden, bytes_accessed=4 * tokens * width, transcendentals=tokens * hidden),
        name="backward_last",
    )(h, dy, *whole, *(t.reshape(side, side, *s) for t, s in zip(later, late, strict=True)))
    return found[:3], found[3:]


def adamw(w, m, v, g):
    m = 0.9 * m + 0.1 * g
    v = 0.95 * v + 0.05 * g * g
    step = m * lax.rsqrt(v + 1e-8) + 0.1 * w
    return (w - 0.02 * step).astype(BF), m, v


def solution(mesh):
    side = math.isqrt(mesh.shape["dp"])

    def step(x, dy, *arrays):
        weights, m, v = (arrays[i : i + 3] for i in (0, 3, 6))
        h = x[0]
        flat = lambda wholes: [w.reshape(-1, w.shape[-1]) for w in wholes]
        low = flat(gather(side, 0, weights[:2], 1))
        above, down, high = forward(side, h, low, weights, 1, 2)
        low += flat([down])
        dh, terms, early = backward_carry(side, above, dy[0], flat(high), 4)
        first, second = backward_last(side, h, dh, low, terms, 3)
        mine = [first, [jnp.concatenate(pair, 1) for pair in zip(early, second[:2], strict=True)] + [second[2]]]
        gradients = [jnp.stack([mine[number][i] for number in range(2)]).astype(F32) for i in range(3)]
        new = [adamw(w.astype(F32), m, v, g) for w, m, v, g in zip(weights, m, v, gradients, strict=True)]
        return tuple(one[which] for which in range(3) for one in new)

    states, cut = P(("rep", "dp"), None, None), P(None, "dp", None)
    return jax.shard_map(
        step,
        mesh=mesh,
        in_specs=(states, states) + (cut,) * 9,
        out_specs=(P("rep", "dp", None),) * 9,
        check_vma=False,
    )
```
